128 devices in a mesh: seq: 8 (over x, core), tensor: 4 (over z), bucket: 4 (over y).
Axes of the slice: x: 4, y: 4, z: 4, core: 2. Of those that a mesh axis runs over, the one named last changes fastest.
Arguments:
- queries: bfloat16 [4, 4096, 3072], P('bucket', ('seq', 'tensor')), may hold values from -6 to 6
- keys: bfloat16 [4, 4096, 3072], P('bucket', ('seq', 'tensor')), may hold values from -6 to 6
- values: bfloat16 [4, 4096, 3072], P('bucket', ('seq', 'tensor')), may hold values from -6 to 6
- lengths: int32 [4], P('bucket'), may hold values from 1024 to 4096, as said below
- out_weight: bfloat16 [3072, 3072], P(('seq', 'bucket'), 'tensor'), may hold values from -0.109375 to 0.109375
Outputs:
- projected: bfloat16 [4, 4096, 3072], P('bucket', ('seq', 'tensor'))
The draws below stay inside these ranges and needn't reach their ends.
Inputs may be any that keep to these rules, and one draw needn't show every extreme that they name: `lengths`: each bucket has 1024 to 4096 live tokens, and at least one bucket has all 4096.
All inputs are finite; a program needn't handle non-finite values.
Results may differ from the reference program's by a relative error of at most 0.018.
Values may be sent and summed in bfloat16 or wider, within the bound.
A program may use at most 128 MiB of HBM per device.

```python
import jax
import jax.numpy as jnp
from jax import lax

D = 3072
HEADS = 24
HS = 128
LEN = 4096
BUCKETS = 4


def draw_queries(key, part):
    drawn = jax.random.normal(jax.random.fold_in(key, 1), (BUCKETS, LEN, D), jnp.float32)
    return jnp.clip(drawn, -6.0, 6.0).astype(jnp.bfloat16)


def draw_keys(key, part):
    drawn = jax.random.normal(jax.random.fold_in(key, 2), (BUCKETS, LEN, D), jnp.float32)
    return jnp.clip(drawn, -6.0, 6.0).astype(jnp.bfloat16)


def draw_lengths(key, part):
    drawn = jax.random.randint(jax.random.fold_in(key, 3), (BUCKETS,), LEN // 4, LEN + 1)
    fullest = jax.random.randint(jax.random.fold_in(key, 4), (), 0, BUCKETS)
    return jnp.where(jnp.arange(BUCKETS) == fullest, LEN, drawn).astype(jnp.int32)


def block_levels(rng, dims, pieces, low, top_value):
    level, own = 1.0, jax.random.fold_in(rng, 6)
    for position, parts in pieces:
        steps = jnp.exp(jax.random.uniform(jax.random.fold_in(own, position), (parts,), jnp.float32, low / len(pieces), top_value / len(pieces)))
        level = level * jnp.repeat(steps, dims[position] // parts).reshape([-1 if axis == position else 1 for axis in range(len(dims))])
    return level


def gaussian(rng, extent, width, limit, cuts=(), held_as=jnp.bfloat16):
    result = jax.random.normal(rng, extent, jnp.float32) * width
    if len(cuts) > 0:
        result = block_levels(rng, extent, cuts, -0.22, 0.18) * result
    return jnp.clip(result, min=-limit, max=limit).astype(held_as)


def setup_inputs(seed: int = 0) -> dict:
    key_list = jax.random.split(jax.random.key(seed), 6)
    queries = draw_queries(jax.random.fold_in(key_list[5], 71), 0)
    keys = draw_keys(jax.random.fold_in(key_list[5], 71), 0)
    values = gaussian(key_list[2], (BUCKETS, LEN, D), 1.0, 6.0, ((0, 4), (1, 32)))
    lengths = draw_lengths(jax.random.fold_in(key_list[5], 71), 0)
    out_weight = gaussian(key_list[4], (D, D), D ** -0.5, 0.109375, ((0, 32), (1, 4)))
    return {"queries": queries, "keys": keys, "values": values, "lengths": lengths, "out_weight": out_weight}


MASKED_SCORE = -1e30


def attend_head(query_head, key_head, value_head, usable):
    scores = jnp.dot(query_head, key_head.T, preferred_element_type=jnp.float32) * (HS ** -0.5)
    scores = jnp.where(usable[None, :], scores, MASKED_SCORE)
    row_peak = jnp.max(scores, axis=-1, keepdims=True)
    exponent = jnp.where(usable[None, :], jnp.exp(scores - row_peak), 0.0)
    numerator = jnp.dot(exponent.astype(jnp.bfloat16), value_head, preferred_element_type=jnp.float32)
    return numerator / jnp.sum(exponent, axis=-1, keepdims=True)


def reference(queries, keys, values, lengths, out_weight):
    def split_heads(array):
        return array.reshape(LEN, HEADS, HS).transpose(1, 0, 2)

    def one_bucket(inputs):
        bucket_q, bucket_k, bucket_v, live_len = inputs
        positions = jnp.arange(LEN, dtype=jnp.int32)
        usable = positions < live_len

        def one_head(trio):
            return attend_head(trio[0], trio[1], trio[2], usable)

        attended = lax.map(one_head, (split_heads(bucket_q), split_heads(bucket_k), split_heads(bucket_v)))
        mixed = attended.transpose(1, 0, 2).reshape(LEN, D)
        mixed = jnp.where(usable[:, None], mixed, 0.0).astype(jnp.bfloat16)
        return jnp.dot(mixed, out_weight, preferred_element_type=jnp.float32).astype(jnp.bfloat16)

    return lax.map(one_bucket, (queries, keys, values, lengths))
```

```python
import functools
import math

import jax
import jax.numpy as jnp
from jax import lax
from jax.experimental import pallas as pl
from jax.experimental.pallas import tpu as pltpu
from jax.sharding import PartitionSpec as P

HS = 128
T = 128
MESH = pl.DeviceIdType.MESH
LOG2E_SCALED = math.log2(math.e) / math.sqrt(HS)
DEAD = -1e30
STEPS = 12


def place(z):
    inner = jnp.where((z == 1) | (z == 2), 1, 0)
    return inner * 2 + z // 2


def attend_kernel(
    len_ref, q_hbm, k_hbm, v_hbm, att_hbm,
    qb, kvb, ob, peak, acc, bias,
    q_send, kv_send, mate_send, part_send, o_send,
    q_recv, kv_recv, mate_recv, part_recv, o_recv,
):
    s, z, y = lax.axis_index("seq"), lax.axis_index("tensor"), lax.axis_index("bucket")
    x, c = s // 2, s % 2
    p = z // 2
    mate_z = p * 2 + 1 - z % 2
    own_base = jnp.where((z == 1) | (z == 2), 2, 0)
    my_block = s * 4 + place(z)

    def push(j, dx, cross):
        xd = (x + dx) % 4
        pd, zd = (p, z) if cross == 0 else (1 - p, 3 - z)
        col = pl.multiple_of(((xd * 2 + pd) * 3 + j) * HS, HS)
        dev = (xd * 2 + c, zd, y)
        slot = dx * 2 + cross
        rows = pl.ds(pl.multiple_of(slot * T, T), T)
        cols = pl.ds(col, HS)
        moves = (
            (q_hbm.at[0, :, cols], qb.at[j, rows], q_send.at[j, slot], q_recv.at[j]),
            (k_hbm.at[0, :, cols], kvb.at[j, my_block, 0], kv_send.at[j, slot, 0], kv_recv.at[j, dx]),
            (v_hbm.at[0, :, cols], kvb.at[j, my_block, 1], kv_send.at[j, slot, 1], kv_recv.at[j, dx]),
        )
        return moves, dev

    def start(j, dx, cross, which):
        moves, dev = push(j, dx, cross)

        def far():
            for w in which:
                src, dst, ss, rs = moves[w]
                pltpu.make_async_remote_copy(src, dst, ss, rs, device_id=dev, device_id_type=MESH).start()

        def near():
            for w in which:
                src, dst, ss, rs = moves[w]
                pltpu.make_async_copy(src, dst, rs).start()

        if cross == 1:
            far()
        else:
            pl.when(dx == 0)(near)
            pl.when(dx != 0)(far)

    @pl.loop(0, 3)
    def _(j):
        @pl.loop(0, 4)
        def _(dx):
            for cross in range(2):
                start(j, dx, cross, (0,))

        @pl.loop(0, 4)
        def _(dx):
            for cross in range(2):
                start(j, dx, cross, (1, 2))

    for sp in range(8):
        lane = lax.broadcasted_iota(jnp.int32, (8, 512), 1)
        quarter = lane // T
        zz = jnp.where(quarter == 0, 0, jnp.where(quarter == 1, 3, quarter - 1))
        token = (sp * 4 + zz) * T + lane % T
        bias[sp] = jnp.where(token < len_ref[0], 0.0, DEAD).astype(jnp.float32)

    def chunk(n, core):
        j, dx = n // 4, n % 4
        return j, dx, ((x - dx + 4) % 4) * 2 + core

    def mate_copy(n):
        j, dx, sp = chunk(n, c)
        part = kvb.at[j, pl.ds(sp * 4 + own_base, 2)]
        return pltpu.make_async_remote_copy(part, part, mate_send.at[n], mate_recv.at[n], device_id=(s, mate_z, y), device_id_type=MESH)

    def part_copy(n):
        j, dx, sp = chunk(n, c)
        part = kvb.at[j, pl.ds(sp * 4, 4)]
        return pltpu.make_async_remote_copy(part, part, part_send.at[n], part_recv.at[n], device_id=(x * 2 + 1 - c, z, y), device_id_type=MESH)

    def relay_to_mate(n):
        j, dx, sp = chunk(n, c)
        part = kvb.at[j, pl.ds(sp * 4 + own_base, 2)]
        pltpu.make_async_copy(part, part, kv_recv.at[j, dx]).wait()
        mate_copy(n).start()

    def relay_to_partner(n):
        mate_copy(n).wait_recv()
        part_copy(n).start()

    def attend(j, sp):
        k = kvb[j, pl.ds(sp * 4, 4), 0].reshape(512, HS)
        v = kvb[j, pl.ds(sp * 4, 4), 1].reshape(512, HS)
        scores = lax.dot_general(qb[j], k, (((1,), (1,)), ((), ())), preferred_element_type=jnp.float32)
        scores = scores + bias[sp, 0:1, :]
        old = peak[...]
        new = jnp.maximum(old, jnp.max(scores, axis=1, keepdims=True))
        weights = jnp.exp2((scores - new) * LOG2E_SCALED)
        rescale = jnp.exp2((old - new) * LOG2E_SCALED)
        wide = jnp.concatenate([v, jnp.ones_like(v)], axis=1)
        acc[...] = acc[...] * rescale + jnp.dot(weights.astype(jnp.bfloat16), wide, preferred_element_type=jnp.float32)
        peak[...] = new

    def o_copies(j, dx, cross):
        xs = (x - dx + 4) % 4
        zs = z if cross == 0 else 3 - z
        slot = dx * 2 + cross
        src = ob.at[j, pl.ds(pl.multiple_of(slot * T, T), T)]
        dst = att_hbm.at[:, pl.ds(pl.multiple_of(((x * 2 + p) * 3 + j) * HS, HS), HS)]
        far = pltpu.make_async_remote_copy(src, dst, o_send.at[j, slot], o_recv.at[j], device_id=(xs * 2 + c, zs, y), device_id_type=MESH)
        near = pltpu.make_async_copy(src, dst, o_recv.at[j])
        return far, near

    relay_to_mate(0)
    relay_to_mate(1)
    relay_to_partner(0)

    @pl.loop(0, STEPS)
    def _(n):
        j, dx = n // 4, n % 4

        @pl.when(n + 2 < STEPS)
        def _():
            relay_to_mate(n + 2)

        @pl.when(n + 1 < STEPS)
        def _():
            relay_to_partner(n + 1)

        @pl.when(dx == 0)
        def _():
            pltpu.make_async_copy(qb.at[j], qb.at[j], q_recv.at[j]).wait()
            peak[...] = jnp.full(peak.shape, DEAD, jnp.float32)
            acc[...] = jnp.zeros_like(acc)

        part_copy(n).wait_recv()

        @pl.loop(0, 2)
        def _(half):
            core = lax.rem(c + half, 2)
            attend(j, ((x - dx + 4) % 4) * 2 + core)

        @pl.when(dx == 3)
        def _():
            ob[j] = (acc[:, :HS] / acc[:, HS:]).astype(jnp.bfloat16)

            @pl.loop(0, 4)
            def _(e):
                for cross in range(2):
                    far, near = o_copies(j, e, cross)
                    if cross == 1:
                        far.start()
                    else:
                        pl.when(e == 0)(lambda near=near: near.start())
                        pl.when(e != 0)(lambda far=far: far.start())

    @pl.loop(0, 3)
    def _(j):
        @pl.loop(0, 4)
        def _(dx):
            for cross in range(2):
                moves, dev = push(j, dx, cross)
                far, near = o_copies(j, dx, cross)

                def drain(moves=moves, dev=dev, far=far):
                    for src, dst, ss, rs in moves:
                        pltpu.make_async_remote_copy(src, dst, ss, rs, device_id=dev, device_id_type=MESH).wait_send()
                    far.wait_send()

                if cross == 1:
                    drain()
                else:
                    pl.when(dx != 0)(drain)
        whole = ob.at[j]
        pltpu.make_async_copy(whole, whole, o_recv.at[j]).wait()

    @pl.loop(0, STEPS)
    def _(n):
        mate_copy(n).wait_send()
        part_copy(n).wait_send()


def attend_all(lengths, queries, keys, values):
    anywhere = pl.BlockSpec(memory_space=pl.ANY)
    dma = pltpu.SemaphoreType.DMA
    return pl.pallas_call(
        attend_kernel,
        out_shape=jax.ShapeDtypeStruct((T, 24 * HS), jnp.bfloat16),
        in_specs=[pl.BlockSpec(memory_space=pltpu.SMEM), anywhere, anywhere, anywhere],
        out_specs=anywhere,
        scratch_shapes=[
            pltpu.VMEM((3, 8 * T, HS), jnp.bfloat16),
            pltpu.VMEM((3, 32, 2, T, HS), jnp.bfloat16),
            pltpu.VMEM((3, 8 * T, HS), jnp.bfloat16),
            pltpu.VMEM((8 * T, 1), jnp.float32),
            pltpu.VMEM((8 * T, 2 * HS), jnp.float32),
            pltpu.VMEM((8, 8, 512), jnp.float32),
            dma((3, 8)), dma((3, 8, 2)), dma((STEPS,)), dma((STEPS,)), dma((3, 8)),
            dma((3,)), dma((3, 4)), dma((STEPS,)), dma((STEPS,)), dma((3,)),
        ],
        compiler_params=pltpu.CompilerParams(vmem_limit_bytes=56 * 2**20, has_side_effects=True),
        cost_estimate=pl.CostEstimate(flops=13 * 10**9, bytes_accessed=20 * 2**20, transcendentals=0),
        name="attend",
    )(lengths, queries, keys, values)


def shards(queries, keys, values, lengths, out_weight):
    s, z = lax.axis_index("seq"), lax.axis_index("tensor")
    weight = lax.all_gather(out_weight, ("seq", "bucket"), axis=0, tiled=True)
    weight = lax.all_gather(weight, "tensor", axis=1, tiled=True)
    attended = attend_all(lengths, queries, keys, values)
    token = (s * 4 + z) * T + jnp.arange(T, dtype=jnp.int32)
    attended = jnp.where((token < lengths[0])[:, None], attended, jnp.bfloat16(0))
    out = jnp.dot(attended, weight, preferred_element_type=jnp.float32)
    return out.astype(jnp.bfloat16)[None]


def solution(mesh):
    tokens = P("bucket", ("seq", "tensor"), None)
    return jax.shard_map(
        shards,
        mesh=mesh,
        in_specs=(tokens, tokens, tokens, P("bucket"), P(("seq", "bucket"), "tensor")),
        out_specs=tokens,
        check_vma=False,
    )
```

```python
import functools
import math

import jax
import jax.numpy as jnp
from jax import lax
from jax.experimental import pallas as pl
from jax.experimental.pallas import tpu as pltpu
from jax.sharding import PartitionSpec as P

HS = 128
T = 128
D = 3072
MESH = pl.DeviceIdType.MESH
LOG2E_SCALED = math.log2(math.e) / math.sqrt(HS)
DEAD = -1e30
STEPS = 12
ROWS_AT_ONCE = 128
GROUPS = (
    (0, 256, "zxy"),
    (256, 256, "zxy"),
    (512, 128, "yzx"),
    (640, 128, "xyz"),
)


def place(z):
    inner = jnp.where((z == 1) | (z == 2), 1, 0)
    return inner * 2 + z // 2


def kernel(
    len_ref, q_hbm, k_hbm, v_hbm, w_hbm, out_hbm,
    qb, kvb, ob, peak, acc, bias, wb, ox, mine, theirs, landed, out_vm,
    q_send, kv_send, mate_send, own_send, part_send, o_send, w_send, sum_send,
    q_recv, kv_recv, mate_recv, part_recv, o_recv, w_recv, sum_recv, w_own, out_sem,
):
    s, z, y = lax.axis_index("seq"), lax.axis_index("tensor"), lax.axis_index("bucket")
    x, c = s // 2, s % 2
    p = z // 2
    mate_z = p * 2 + 1 - z % 2
    partner = (x * 2 + 1 - c, z, y)
    own_base = jnp.where((z == 1) | (z == 2), 2, 0)
    my_block = s * 4 + place(z)

    def remote(src, dst, ss, rs, dev):
        return pltpu.make_async_remote_copy(src, dst, ss, rs, device_id=dev, device_id_type=MESH)

    barrier = pltpu.get_barrier_semaphore()
    peers = [((x + dx) % 4 * 2 + c, zz, y) for dx in range(4) for zz in (z, 3 - z) if not (dx == 0 and zz is z)]
    peers += [((x + dx) % 4 * 2 + 1 - c, zz, y) for dx in range(4) for zz in (z, 3 - z)]
    peers += [(s, (z + d) % 4, y) for d in (1, 2, 3)] + [(s, z, (y + d) % 4) for d in (1, 2, 3)]
    for dev in peers:
        pl.semaphore_signal(barrier, inc=1, device_id=dev, device_id_type=MESH)
    pl.semaphore_wait(barrier, len(peers))

    def q_move(j, dx, cross):
        xd = (x + dx) % 4
        pd, zd = (p, z) if cross == 0 else (1 - p, 3 - z)
        cols = pl.ds(pl.multiple_of(((xd * 2 + pd) * 3 + j) * HS, HS), HS)
        slot = dx * 2 + cross
        rows = pl.ds(pl.multiple_of(slot * T, T), T)
        return (q_hbm.at[0, :, cols], qb.at[j, rows], q_send.at[j, slot], q_recv.at[j], (xd * 2 + c, zd, y))

    def kv_move(j, dx, cross, which):
        xd = (x + dx) % 4
        pd, zd = (p, z) if cross == 0 else (1 - p, 3 - z)
        cols = pl.ds(pl.multiple_of(((xd * 2 + pd) * 3 + j) * HS, HS), HS)
        src = (k_hbm, v_hbm)[which].at[0, :, cols]
        return (src, kvb.at[j, my_block, which], kv_send.at[j, dx * 2 + cross, which], kv_recv.at[j, dx], (xd * 2 + c, zd, y))

    def own_to_mate(j, which):
        cols = pl.ds(pl.multiple_of(((x * 2 + p) * 3 + j) * HS, HS), HS)
        src = (k_hbm, v_hbm)[which].at[0, :, cols]
        return remote(src, kvb.at[j, my_block, which], own_send.at[j, which], mate_recv.at[j * 4], (s, mate_z, y))

    def begin(move, dx, cross):
        def far():
            remote(*move).start()

        def near():
            pltpu.make_async_copy(move[0], move[1], move[3]).start()

        if cross == 1:
            far()
        elif isinstance(dx, int):
            (near if dx == 0 else far)()
        else:
            pl.when(dx == 0)(near)
            pl.when(dx != 0)(far)

    def begin_kv(j, dx):
        for cross in range(2):
            for which in range(2):
                begin(kv_move(j, dx, cross, which), dx, cross)

    def begin_q(j):
        @pl.loop(0, 4)
        def _(dx):
            for cross in range(2):
                begin(q_move(j, dx, cross), dx, cross)

    at = {"x": x, "y": y, "z": z}

    def shifted(axis, d):
        to = dict(at)
        to[axis] = (at[axis] + d + 4) % 4
        return to

    def device(to):
        return (to["x"] * 2 + c, to["z"], to["y"])

    def slab(g, have, to, half=None):
        first, count, _ = GROUPS[g]
        split = "z" if "x" not in have else "x"
        pick = lambda axis: (
            (pl.ds(half * 2, 2) if half is not None and axis == split else pl.ds(0, 4)) if axis in have else to[axis]
        )
        rows = pl.ds(0, 384) if "y" in have else pl.ds(pl.multiple_of(to["y"] * 96, 32), 96)
        return wb.at[pick("x"), pick("z"), rows, pl.ds(first, count)]

    def w_copy(g, stage, d, half=None):
        first, count, order = GROUPS[g]
        axis, have = order[stage], order[:stage]
        whose = at if half is None else shifted(axis, -d)
        region = slab(g, have, whose, half)
        src = w_hbm.at[:, pl.ds(first, count)] if stage == 0 else region
        index = stage * 3 + d - 1 if stage < 2 else 6 + (0 if d == 1 else 1) + (0 if half is None else 2)
        return remote(src, region, w_send.at[g, index], w_recv.at[g, index], device(shifted(axis, d)))

    def w_begin(g, stage):
        for d in (1, 3, 2) if stage < 2 else (1, 3):
            w_copy(g, stage, d).start()

    def w_arrived(g, stage):
        for d in (1, 3, 2) if stage < 2 else (1, 3):
            w_copy(g, stage, d).wait_recv()

    def w_pass_on(g):
        w_copy(g, 2, 1, 0).start()
        w_copy(g, 2, 3, 1).start()

    def w_complete(g):
        w_copy(g, 2, 1, 0).wait_recv()
        w_copy(g, 2, 3, 1).wait_recv()

    def w_drain(g):
        for stage in range(3):
            for d in (1, 3, 2) if stage < 2 else (1, 3):
                w_copy(g, stage, d).wait_send()
        w_copy(g, 2, 1, 0).wait_send()
        w_copy(g, 2, 3, 1).wait_send()

    w_mine = pltpu.make_async_copy(w_hbm, wb.at[x, z, pl.ds(pl.multiple_of(y * 96, 32), 96)], w_own)

    begin_kv(0, 0)
    for which in range(2):
        own_to_mate(0, which).start()
    w_mine.start()
    begin_kv(0, 1)
    for g in range(2):
        w_begin(g, 0)
    begin_q(0)
    begin_kv(0, 2)
    begin_kv(0, 3)
    for j in (1, 2):
        for which in range(2):
            own_to_mate(j, which).start()
    for g in range(2, len(GROUPS)):
        w_begin(g, 0)

    @pl.loop(1, 3)
    def _(j):
        @pl.loop(0, 4)
        def _(dx):
            begin_kv(j, dx)

        begin_q(j)

    for sp in range(8):
        lane = lax.broadcasted_iota(jnp.int32, (8, 512), 1)
        quarter = lane // T
        zz = jnp.where(quarter == 0, 0, jnp.where(quarter == 1, 3, quarter - 1))
        token = (sp * 4 + zz) * T + lane % T
        bias[sp] = jnp.where(token < len_ref[0], 0.0, DEAD).astype(jnp.float32)

    def chunk(n):
        j, dx = n // 4, n % 4
        return j, dx, ((x - dx + 4) % 4) * 2 + c

    def mate_copy(n):
        j, dx, sp = chunk(n)
        part = kvb.at[j, pl.ds(sp * 4 + own_base, 2)]
        return remote(part, part, mate_send.at[n], mate_recv.at[n], (s, mate_z, y))

    def cross_copy(n):
        j, dx, sp = chunk(n)
        part = kvb.at[j, sp * 4 + place(3 - z)]
        return remote(part, part, mate_send.at[n], mate_recv.at[n], (s, mate_z, y))

    def part_copy(n):
        j, dx, sp = chunk(n)
        part = kvb.at[j, pl.ds(sp * 4, 4)]
        return remote(part, part, part_send.at[n], part_recv.at[n], partner)

    def relay_to_mate(n):
        j, dx, sp = chunk(n)
        part = kvb.at[j, pl.ds(sp * 4 + own_base, 2)]
        pltpu.make_async_copy(part, part, kv_recv.at[j, dx]).wait()

        def all_of_it():
            mate_copy(n).start()

        def the_rest():
            cross_copy(n).start()

        if isinstance(dx, int):
            (the_rest if dx == 0 else all_of_it)()
        else:
            pl.when(dx == 0)(the_rest)
            pl.when(dx != 0)(all_of_it)

    def relay_to_partner(n):
        mate_copy(n).wait_recv()
        part_copy(n).start()

    def attend(j, dx):
        base = ((x - dx + 4) % 4) * 8
        k = kvb[j, pl.ds(base, 8), 0].reshape(1024, HS)
        v = kvb[j, pl.ds(base, 8), 1].reshape(1024, HS)
        wide = jnp.concatenate([v, jnp.ones_like(v)], axis=1)
        both = (x - dx + 4) % 4 * 2
        dead = jnp.concatenate([bias[both, 0:1, :], bias[both + 1, 0:1, :]], axis=1)
        for first in range(0, 8 * T, ROWS_AT_ONCE):
            r = pl.ds(first, ROWS_AT_ONCE)
            scores = lax.dot_general(qb[j, r], k, (((1,), (1,)), ((), ())), preferred_element_type=jnp.float32) + dead
            old = peak[r, :]
            new = jnp.maximum(old, jnp.max(scores, axis=1, keepdims=True))
            weights = jnp.exp2((scores - new) * LOG2E_SCALED).astype(jnp.bfloat16)
            rescale = jnp.exp2((old - new) * LOG2E_SCALED)
            acc[r, :] = acc[r, :] * rescale + jnp.dot(weights, wide, preferred_element_type=jnp.float32)
            peak[r, :] = new

    def o_move(j, dx, cross):
        xs = (x - dx + 4) % 4
        zs = z if cross == 0 else 3 - z
        slot = dx * 2 + cross
        src = ob.at[j, pl.ds(pl.multiple_of(slot * T, T), T)]
        dst = ox.at[pl.ds(pl.multiple_of(c * T, T), T), pl.ds(pl.multiple_of((x * 3 + j) * HS, HS), HS)]
        return src, dst, o_send.at[j, slot], o_recv.at[j], (xs * 2 + p, zs, y)

    def send_attended(j):
        @pl.loop(0, 4)
        def _(dx):
            for cross in range(2):
                move = o_move(j, dx, cross)

                def far(move=move):
                    remote(*move).start()

                def near(move=move):
                    pltpu.make_async_copy(move[0], move[1], move[3]).start()

                if cross == 1:
                    far()
                else:
                    pl.when((dx == 0) & (p == c))(near)
                    pl.when((dx != 0) | (p != c))(far)

    relay_to_mate(0)
    for g in range(2):
        w_arrived(g, 0)
    w_mine.wait()
    for g in range(2):
        w_begin(g, 1)
    relay_to_mate(1)
    relay_to_partner(0)

    events = {
        1: lambda: (w_arrived(0, 1), w_begin(0, 2), w_arrived(1, 1), w_begin(1, 2)),
        2: lambda: (w_arrived(2, 0), w_begin(2, 1), w_arrived(3, 0), w_begin(3, 1)),
        6: lambda: (w_arrived(2, 1), w_begin(2, 2), w_arrived(3, 1), w_begin(3, 2)),
        9: lambda: (w_arrived(0, 2), w_pass_on(0)),
    }

    @pl.loop(0, STEPS)
    def _(n):
        j, dx = n // 4, n % 4

        @pl.when(n + 2 < STEPS)
        def _():
            relay_to_mate(n + 2)

        @pl.when(n + 1 < STEPS)
        def _():
            relay_to_partner(n + 1)

        for when, event in events.items():
            pl.when(n == when)(lambda event=event: event() and None)

        @pl.when(dx == 0)
        def _():
            pltpu.make_async_copy(qb.at[j], qb.at[j], q_recv.at[j]).wait()
            peak[...] = jnp.full(peak.shape, DEAD, jnp.float32)
            acc[...] = jnp.zeros_like(acc)

        part_copy(n).wait_recv()
        attend(j, dx)

        @pl.when(dx == 3)
        def _():
            ob[j] = (acc[:, :HS] / acc[:, HS:]).astype(jnp.bfloat16)
            send_attended(j)

    w_arrived(2, 2)
    w_pass_on(2)
    w_arrived(3, 2)
    w_pass_on(3)
    w_arrived(1, 2)
    w_pass_on(1)

    for j in range(3):
        part = ob.at[j]
        pltpu.make_async_copy(part, part, o_recv.at[j]).wait()

    def sum_copy(g, zb):
        first, count, _ = GROUPS[g]
        cols = pl.ds(pl.multiple_of(zb * 768 + first, HS), count)
        return remote(theirs.at[:, cols], landed.at[:, cols], sum_send.at[g, zb], sum_recv.at[g, zb], partner)

    order = (2, 3, 0, 1)
    for g in order:
        w_complete(g)
        first, count, _ = GROUPS[g]

        @pl.loop(0, 4)
        def _(zb, first=first, count=count, g=g):
            cols = pl.ds(pl.multiple_of(zb * 768 + first, HS), count)
            total = jnp.zeros((2 * T, count), jnp.float32)
            for xb in range(4):
                total += jnp.dot(
                    ox[:, xb * 384 : (xb + 1) * 384], wb[xb, zb, :, first : first + count], preferred_element_type=jnp.float32
                )
            low, high = total[:T], total[T:]
            mine[:, cols] = jnp.where(c == 0, low, high)
            theirs[:, cols] = jnp.where(c == 0, high, low)
            sum_copy(g, zb).start()

    token = (s * 4 + z) * T + lax.broadcasted_iota(jnp.int32, (T, 1), 0)
    live = token < len_ref[0]
    for g in order:
        first, count, _ = GROUPS[g]

        @pl.loop(0, 4)
        def _(zb, first=first, count=count, g=g):
            cols = pl.ds(pl.multiple_of(zb * 768 + first, HS), count)
            sum_copy(g, zb).wait_recv()
            out_vm[:, cols] = jnp.where(live, mine[:, cols] + landed[:, cols], 0.0).astype(jnp.bfloat16)

    done = pltpu.make_async_copy(out_vm, out_hbm.at[0], out_sem)
    done.start()

    @pl.loop(0, 3)
    def _(j):
        for which in range(2):
            own_to_mate(j, which).wait_send()

        @pl.loop(0, 4)
        def _(dx):
            for cross in range(2):
                moves = [q_move(j, dx, cross), kv_move(j, dx, cross, 0), kv_move(j, dx, cross, 1)]
                o = o_move(j, dx, cross)

                def drain(moves=moves):
                    for move in moves:
                        remote(*move).wait_send()

                def drain_o(o=o):
                    remote(*o).wait_send()

                if cross == 1:
                    drain()
                    drain_o()
                else:
                    pl.when(dx != 0)(drain)
                    pl.when((dx != 0) | (p != c))(drain_o)

    @pl.loop(0, STEPS)
    def _(n):
        pl.when(n % 4 == 0)(lambda: cross_copy(n).wait_send())
        pl.when(n % 4 != 0)(lambda: mate_copy(n).wait_send())
        part_copy(n).wait_send()

    for g in range(len(GROUPS)):
        w_drain(g)

        @pl.loop(0, 4)
        def _(zb, g=g):
            sum_copy(g, zb).wait_send()

    done.wait()


def everything(lengths, queries, keys, values, weight):
    anywhere = pl.BlockSpec(memory_space=pl.ANY)
    dma = pltpu.SemaphoreType.DMA
    bf16, f32, vmem = jnp.bfloat16, jnp.float32, pltpu.VMEM
    groups = len(GROUPS)
    return pl.pallas_call(
        kernel,
        out_shape=jax.ShapeDtypeStruct((1, T, D), bf16),
        in_specs=[pl.BlockSpec(memory_space=pltpu.SMEM)] + [anywhere] * 4,
        out_specs=anywhere,
        scratch_shapes=[
            vmem((3, 8 * T, HS), bf16),
            vmem((3, 32, 2, T, HS), bf16),
            vmem((3, 8 * T, HS), bf16),
            vmem((8 * T, 1), f32),
            vmem((8 * T, 2 * HS), f32),
            vmem((8, 8, 512), f32),
            vmem((4, 4, 384, 768), bf16),
            vmem((2 * T, 1536), bf16),
            vmem((T, D), f32),
            vmem((T, D), f32),
            vmem((T, D), f32),
            vmem((T, D), bf16),
            dma((3, 8)), dma((3, 8, 2)), dma((STEPS,)), dma((3, 2)), dma((STEPS,)), dma((3, 8)), dma((groups, 10)), dma((groups, 4)),
            dma((3,)), dma((3, 4)), dma((STEPS,)), dma((STEPS,)), dma((3,)), dma((groups, 10)), dma((groups, 4)), dma(()), dma(()),
        ],
        compiler_params=pltpu.CompilerParams(vmem_limit_bytes=60 * 2**20, has_side_effects=True, collective_id=0),
        cost_estimate=pl.CostEstimate(flops=16 * 10**9, bytes_accessed=30 * 2**20, transcendentals=0),
        name="attend",
    )(lengths, queries, keys, values, weight)


def shards(queries, keys, values, lengths, out_weight):
    return everything(lengths, queries, keys, values, out_weight)


def solution(mesh):
    tokens = P("bucket", ("seq", "tensor"), None)
    return jax.shard_map(
        shards,
        mesh=mesh,
        in_specs=(tokens, tokens, tokens, P("bucket"), P(("seq", "bucket"), "tensor")),
        out_specs=tokens,
        check_vma=False,
    )
```

```python
import functools
import math

import jax
import jax.numpy as jnp
from jax import lax
from jax.experimental import pallas as pl
from jax.experimental.pallas import tpu as pltpu
from jax.sharding import PartitionSpec as P

HS = 128
T = 128
D = 3072
MESH = pl.DeviceIdType.MESH
LOG2E_SCALED = math.log2(math.e) / math.sqrt(HS)
DEAD = -1e30
STEPS = 12
ROWS_AT_ONCE = 128
RINGS = 2
GROUPS = (
    (0, 256, "zxy"),
    (256, 256, "xzy"),
    (512, 128, "yzx"),
    (640, 128, "xyz"),
)


def place(z):
    inner = jnp.where((z == 1) | (z == 2), 1, 0)
    return inner * 2 + z // 2


def kernel(
    len_ref, q_hbm, k_hbm, v_hbm, w_hbm, out_hbm,
    qb, kvb, ob, peak, acc, bias, wb, ox, mine, theirs, landed, out_vm,
    q_send, kv_send, mate_send, own_send, part_send, o_send, w_send, sum_send,
    q_recv, kv_recv, mate_recv, part_recv, o_recv, w_recv, r_recv, sum_recv, w_own, out_sem,
):
    s, z, y = lax.axis_index("seq"), lax.axis_index("tensor"), lax.axis_index("bucket")
    x, c = s // 2, s % 2
    p = z // 2
    mate_z = p * 2 + 1 - z % 2
    partner = (x * 2 + 1 - c, z, y)
    own_base = jnp.where((z == 1) | (z == 2), 2, 0)
    my_block = s * 4 + place(z)

    def remote(src, dst, ss, rs, dev):
        return pltpu.make_async_remote_copy(src, dst, ss, rs, device_id=dev, device_id_type=MESH)

    barrier = pltpu.get_barrier_semaphore()
    peers = [((x + dx) % 4 * 2 + c, zz, y) for dx in range(4) for zz in (z, 3 - z) if not (dx == 0 and zz is z)]
    peers += [((x + dx) % 4 * 2 + 1 - c, zz, y) for dx in range(4) for zz in (z, 3 - z)]
    peers += [(s, (z + d) % 4, y) for d in (1, 2, 3)] + [(s, z, (y + d) % 4) for d in (1, 2, 3)]
    for dev in peers:
        pl.semaphore_signal(barrier, inc=1, device_id=dev, device_id_type=MESH)
    pl.semaphore_wait(barrier, len(peers))

    def q_move(j, dx, cross):
        xd = (x + dx) % 4
        pd, zd = (p, z) if cross == 0 else (1 - p, 3 - z)
        cols = pl.ds(pl.multiple_of(((xd * 2 + pd) * 3 + j) * HS, HS), HS)
        slot = dx * 2 + cross
        rows = pl.ds(pl.multiple_of(slot * T, T), T)
        return (q_hbm.at[0, :, cols], qb.at[j, rows], q_send.at[j], q_recv.at[j], (xd * 2 + c, zd, y))

    def kv_move(j, dx, cross, which):
        xd = (x + dx) % 4
        pd, zd = (p, z) if cross == 0 else (1 - p, 3 - z)
        cols = pl.ds(pl.multiple_of(((xd * 2 + pd) * 3 + j) * HS, HS), HS)
        src = (k_hbm, v_hbm)[which].at[0, :, cols]
        return (src, kvb.at[j, my_block, which], kv_send.at[j], kv_recv.at[j, dx], (xd * 2 + c, zd, y))

    def own_to_mate(j, which):
        cols = pl.ds(pl.multiple_of(((x * 2 + p) * 3 + j) * HS, HS), HS)
        src = (k_hbm, v_hbm)[which].at[0, :, cols]
        return remote(src, kvb.at[j, my_block, which], own_send, mate_recv.at[j * 4], (s, mate_z, y))

    def begin(move, dx, cross):
        def far():
            remote(*move).start()

        def near():
            pltpu.make_async_copy(move[0], move[1], move[3]).start()

        if cross == 1:
            far()
        elif isinstance(dx, int):
            (near if dx == 0 else far)()
        else:
            pl.when(dx == 0)(near)
            pl.when(dx != 0)(far)

    def begin_kv(j, dx):
        for cross in range(2):
            for which in range(2):
                begin(kv_move(j, dx, cross, which), dx, cross)

    def begin_q(j, dx):
        for cross in range(2):
            begin(q_move(j, dx, cross), dx, cross)

    def begin_chunk(m):
        j, dx = m // 4, m % 4
        begin_kv(j, dx)
        if isinstance(m, int):
            begin_q(j + 1, dx)
        else:
            pl.when(j < 2)(lambda: begin_q(j + 1, dx))

    at = {"x": x, "y": y, "z": z}

    def shifted(axis, d):
        to = dict(at)
        to[axis] = (at[axis] + d + 4) % 4
        return to

    def device(to):
        return (to["x"] * 2 + c, to["z"], to["y"])

    def slab(g, have, to, half=None):
        first, count, _ = GROUPS[g]
        split = "z" if "x" not in have else "x"
        pick = lambda axis: (
            (pl.ds(half * 2, 2) if half is not None and axis == split else pl.ds(0, 4)) if axis in have else to[axis]
        )
        rows = pl.ds(0, 384) if "y" in have else pl.ds(pl.multiple_of(to["y"] * 96, 32), 96)
        return wb.at[pick("x"), pick("z"), rows, pl.ds(first, count)]

    def w_copy(g, stage, d, half=None):
        first, count, order = GROUPS[g]
        axis, have = order[stage], order[:stage]
        whose = at if half is None else shifted(axis, -d)
        region = slab(g, have, whose, half)
        src = w_hbm.at[:, pl.ds(first, count)] if stage == 0 else region
        if stage == 0:
            arrival = 0
        elif stage == 1:
            arrival = d
        else:
            arrival = 4 + (0 if d == 1 else 1) + (0 if half is None else 2)
        return remote(src, region, w_send.at[g, stage + (0 if half is None else 1)], w_recv.at[g, arrival], device(shifted(axis, d)))

    def w_begin(g, stage, ds=None):
        for d in ds or ((1, 3, 2) if stage < 2 else (1, 3)):
            w_copy(g, stage, d).start()

    def w_arrived(g, stage):
        if stage == 0:
            first, count, _ = GROUPS[g]
            three = wb.at[0, 0, pl.ds(0, 288), pl.ds(first, count)]
            pltpu.make_async_copy(three, three, w_recv.at[g, 0]).wait()
        else:
            for d in (1, 3, 2) if stage < 2 else (1, 3):
                w_copy(g, stage, d).wait_recv()

    def w_pass_on(g):
        w_copy(g, 2, 1, 0).start()
        w_copy(g, 2, 3, 1).start()

    def w_complete(g):
        w_copy(g, 2, 1, 0).wait_recv()
        w_copy(g, 2, 3, 1).wait_recv()

    def settle(region, sem):
        pltpu.make_async_copy(region, region, sem).wait()

    def w_drain(g):
        first, count, _ = GROUPS[g]
        settle(wb.at[0, 0, pl.ds(0, 288), pl.ds(0, count)], w_send.at[g, 0])
        settle(wb.at[0, 0, pl.ds(0, 96 * count // 64), :], w_send.at[g, 1])
        settle(wb.at[0, :, pl.ds(0, 256 if g < RINGS else 128), :], w_send.at[g, 2])
        if g < RINGS:
            settle(wb.at[0, :, pl.ds(0, 128), :], w_send.at[g, 3])
        else:
            settle(wb.at[0, 0, pl.ds(0, 256), :], w_send.at[g, 3])

    def ring_copy(g, u, d, onward=False):
        first, count, order = GROUPS[g]
        whose = (y + 4 - d) % 4 if onward else y
        part = pl.ds(0 if d == 1 else 2, 2) if onward else pl.ds(0, 4)
        rows = pl.ds(pl.multiple_of(whose * 96, 32), 96)
        if order[1] == "x":
            region = wb.at[(x + 4 - u) % 4, part, rows, pl.ds(first, count)]
        else:
            region = wb.at[part, (z + 4 - u) % 4, rows, pl.ds(first, count)]
        index = (2 if onward else 0) + (0 if d == 1 else 1)
        return remote(region, region, w_send.at[g, 3 if onward else 2], r_recv.at[g, u, index], (s, z, (y + d) % 4))

    def ring_begin(g, u):
        for d in (1, 3):
            ring_copy(g, u, d).start()

    def ring_pass_on(g, u):
        for d in (1, 3):
            ring_copy(g, u, d).wait_recv()
            ring_copy(g, u, d, True).start()

    def ring_complete(g):
        for u in range(4):
            for d in (1, 3):
                ring_copy(g, u, d, True).wait_recv()

    def slab_arrived(g, *us):
        for u in us:
            w_copy(g, 1, u).wait_recv()
            ring_begin(g, u)

    w_mine = pltpu.make_async_copy(w_hbm, wb.at[x, z, pl.ds(pl.multiple_of(y * 96, 32), 96)], w_own)

    begin_kv(0, 0)
    for which in range(2):
        own_to_mate(0, which).start()
    w_mine.start()
    begin_kv(0, 1)
    for g in range(RINGS):
        w_begin(g, 0)
    for dx in range(4):
        begin_q(0, dx)
    begin_q(1, 0)
    begin_q(1, 1)

    for sp in range(8):
        lane = lax.broadcasted_iota(jnp.int32, (8, 512), 1)
        quarter = lane // T
        zz = jnp.where(quarter == 0, 0, jnp.where(quarter == 1, 3, quarter - 1))
        token = (sp * 4 + zz) * T + lane % T
        bias[sp] = jnp.where(token < len_ref[0], 0.0, DEAD).astype(jnp.float32)

    def chunk(n):
        j, dx = n // 4, n % 4
        return j, dx, ((x - dx + 4) % 4) * 2 + c

    def mate_copy(n):
        j, dx, sp = chunk(n)
        part = kvb.at[j, pl.ds(sp * 4 + own_base, 2)]
        return remote(part, part, mate_send, mate_recv.at[n], (s, mate_z, y))

    def cross_copy(n):
        j, dx, sp = chunk(n)
        part = kvb.at[j, sp * 4 + place(3 - z)]
        return remote(part, part, mate_send, mate_recv.at[n], (s, mate_z, y))

    def part_copy(n):
        j, dx, sp = chunk(n)
        part = kvb.at[j, pl.ds(sp * 4, 4)]
        return remote(part, part, part_send, part_recv.at[n], partner)

    def relay_to_mate(n):
        j, dx, sp = chunk(n)
        part = kvb.at[j, pl.ds(sp * 4 + own_base, 2)]
        pltpu.make_async_copy(part, part, kv_recv.at[j, dx]).wait()

        def all_of_it():
            mate_copy(n).start()

        def the_rest():
            cross_copy(n).start()

        if isinstance(dx, int):
            (the_rest if dx == 0 else all_of_it)()
        else:
            pl.when(dx == 0)(the_rest)
            pl.when(dx != 0)(all_of_it)

    def relay_to_partner(n):
        mate_copy(n).wait_recv()
        part_copy(n).start()

    def attend(j, dx):
        base = ((x - dx + 4) % 4) * 8
        k = kvb[j, pl.ds(base, 8), 0].reshape(1024, HS)
        v = kvb[j, pl.ds(base, 8), 1].reshape(1024, HS)
        wide = jnp.concatenate([v, jnp.ones_like(v)], axis=1)
        both = (x - dx + 4) % 4 * 2
        dead = jnp.concatenate([bias[both, 0:1, :], bias[both + 1, 0:1, :]], axis=1)
        for first in range(0, 8 * T, ROWS_AT_ONCE):
            r = pl.ds(first, ROWS_AT_ONCE)
            scores = lax.dot_general(qb[j, r], k, (((1,), (1,)), ((), ())), preferred_element_type=jnp.float32) + dead
            old = peak[r, :]
            new = jnp.maximum(old, jnp.max(scores, axis=1, keepdims=True))
            weights = jnp.exp2((scores - new) * LOG2E_SCALED).astype(jnp.bfloat16)
            rescale = jnp.exp2((old - new) * LOG2E_SCALED)
            acc[r, :] = acc[r, :] * rescale + jnp.dot(weights, wide, preferred_element_type=jnp.float32)
            peak[r, :] = new

    def o_move(j, dx, cross):
        xs = (x - dx + 4) % 4
        zs = z if cross == 0 else 3 - z
        slot = dx * 2 + cross
        src = ob.at[j, pl.ds(pl.multiple_of(slot * T, T), T)]
        dst = ox.at[pl.ds(pl.multiple_of(jnp.where(p == c, 0, T), T), T), pl.ds(pl.multiple_of((x * 3 + j) * HS, HS), HS)]
        return src, dst, o_send, o_recv.at[j], (xs * 2 + p, zs, y)

    def send_attended(j):
        @pl.loop(0, 4)
        def _(dx):
            for cross in range(2):
                move = o_move(j, dx, cross)

                def far(move=move):
                    remote(*move).start()

                def near(move=move):
                    pltpu.make_async_copy(move[0], move[1], move[3]).start()

                if cross == 1:
                    far()
                else:
                    pl.when((dx == 0) & (p == c))(near)
                    pl.when((dx != 0) | (p != c))(far)

    relay_to_mate(0)
    begin_chunk(2)
    relay_to_mate(1)
    begin_chunk(3)
    w_mine.wait()
    for g in range(RINGS):
        w_arrived(g, 0)
        ring_begin(g, 0)
    relay_to_partner(0)

    def own_heads():
        for j in (1, 2):
            for which in range(2):
                own_to_mate(j, which).start()

    events = {
        0: lambda: (w_begin(0, 1, (1, 3)), w_begin(1, 1, (1,)), own_heads()),
        1: lambda: (w_begin(0, 1, (2,)), w_begin(1, 1, (3,))),
        2: lambda: (w_begin(1, 1, (2,)), ring_pass_on(0, 0), ring_pass_on(1, 0), w_begin(2, 0), w_begin(3, 0)),
        3: lambda: slab_arrived(0, 1, 3),
        4: lambda: (slab_arrived(0, 2), slab_arrived(1, 1)),
        5: lambda: (slab_arrived(1, 3), w_arrived(2, 0), w_begin(2, 1), w_arrived(3, 0), w_begin(3, 1)),
        6: lambda: slab_arrived(1, 2),
        7: lambda: [ring_pass_on(0, u) for u in (1, 3, 2)],
        8: lambda: (w_arrived(2, 1), w_begin(2, 2), w_arrived(3, 1), w_begin(3, 2)),
        11: lambda: (ring_pass_on(1, 1), w_arrived(3, 2), w_pass_on(3)),
    }

    @pl.loop(0, STEPS)
    def _(n):
        j, dx = n // 4, n % 4

        @pl.when(n + 2 < STEPS)
        def _():
            relay_to_mate(n + 2)

        @pl.when(n + 4 < STEPS)
        def _():
            begin_chunk(n + 4)

        @pl.when(n + 1 < STEPS)
        def _():
            relay_to_partner(n + 1)

        for when, event in events.items():
            pl.when(n == when)(lambda event=event: event() and None)

        @pl.when(dx == 0)
        def _():
            pltpu.make_async_copy(qb.at[j], qb.at[j], q_recv.at[j]).wait()
            peak[...] = jnp.full(peak.shape, DEAD, jnp.float32)
            acc[...] = jnp.zeros_like(acc)

        part_copy(n).wait_recv()
        attend(j, dx)

        @pl.when(dx == 3)
        def _():
            ob[j] = (acc[:, :HS] / acc[:, HS:]).astype(jnp.bfloat16)
            send_attended(j)

    for u in (3, 2):
        ring_pass_on(1, u)
    w_arrived(2, 2)
    w_pass_on(2)

    for j in range(3):
        settle(qb.at[0, pl.ds(0, 7 * T)], q_send.at[j])
        settle(kvb.at[0, pl.ds(0, 7)], kv_send.at[j])
    settle(kvb.at[0, pl.ds(0, 3)], own_send)
    settle(kvb.at[0, pl.ds(0, 21)], mate_send)
    settle(kvb.at[:, pl.ds(0, 16)], part_send)

    for j in range(3):
        part = ob.at[j]
        pltpu.make_async_copy(part, part, o_recv.at[j]).wait()

    def sum_copy(g, zb):
        first, count, _ = GROUPS[g]
        cols = pl.ds(pl.multiple_of(zb * 768 + first, HS), count)
        return remote(theirs.at[:, cols], landed.at[:, cols], sum_send, sum_recv.at[g, zb], partner)

    order = (3, 0, 2, 1)
    for g in order:
        (ring_complete if g < RINGS else w_complete)(g)
        first, count, _ = GROUPS[g]

        @pl.loop(0, 4)
        def _(zb, first=first, count=count, g=g):
            cols = pl.ds(pl.multiple_of(zb * 768 + first, HS), count)
            total = jnp.zeros((2 * T, count), jnp.float32)
            for xb in range(4):
                total += jnp.dot(
                    ox[:, xb * 384 : (xb + 1) * 384], wb[xb, zb, :, first : first + count], preferred_element_type=jnp.float32
                )
            mine[:, cols] = total[:T]
            theirs[:, cols] = total[T:]
            sum_copy(g, zb).start()

    for g in order:
        first, count, _ = GROUPS[g]

        @pl.loop(0, 4)
        def _(zb, first=first, count=count, g=g):
            cols = pl.ds(pl.multiple_of(zb * 768 + first, HS), count)
            sum_copy(g, zb).wait_recv()
            out_vm[:, cols] = (mine[:, cols] + landed[:, cols]).astype(jnp.bfloat16)

    done = pltpu.make_async_copy(out_vm, out_hbm.at[0], out_sem)
    done.start()

    pl.when(p == c)(lambda: settle(ob.at[:, pl.ds(0, 7 * T)], o_send))
    pl.when(p != c)(lambda: settle(ob, o_send))
    for g in range(len(GROUPS)):
        w_drain(g)
    settle(landed, sum_send)
    done.wait()


def everything(lengths, queries, keys, values, weight):
    anywhere = pl.BlockSpec(memory_space=pl.ANY)
    dma = pltpu.SemaphoreType.DMA
    bf16, f32, vmem = jnp.bfloat16, jnp.float32, pltpu.VMEM
    groups = len(GROUPS)
    return pl.pallas_call(
        kernel,
        out_shape=jax.ShapeDtypeStruct((1, T, D), bf16),
        in_specs=[pl.BlockSpec(memory_space=pltpu.SMEM)] + [anywhere] * 4,
        out_specs=anywhere,
        scratch_shapes=[
            vmem((3, 8 * T, HS), bf16),
            vmem((3, 32, 2, T, HS), bf16),
            vmem((3, 8 * T, HS), bf16),
            vmem((8 * T, 1), f32),
            vmem((8 * T, 2 * HS), f32),
            vmem((8, 8, 512), f32),
            vmem((4, 4, 384, 768), bf16),
            vmem((2 * T, 1536), bf16),
            vmem((T, D), f32),
            vmem((T, D), f32),
            vmem((T, D), f32),
            vmem((T, D), bf16),
            dma((3,)), dma((3,)), dma(()), dma(()), dma(()), dma(()), dma((groups, 4)), dma(()),
            dma((3,)), dma((3, 4)), dma((STEPS,)), dma((STEPS,)), dma((3,)), dma((groups, 8)), dma((RINGS, 4, 4)), dma((groups, 4)), dma(()), dma(()),
        ],
        compiler_params=pltpu.CompilerParams(vmem_limit_bytes=60 * 2**20, has_side_effects=True, collective_id=0),
        cost_estimate=pl.CostEstimate(flops=16 * 10**9, bytes_accessed=30 * 2**20, transcendentals=0),
        name="attend",
    )(lengths, queries, keys, values, weight)


def shards(queries, keys, values, lengths, out_weight):
    s, z = lax.axis_index("seq"), lax.axis_index("tensor")
    token = (s * 4 + z) * T + jnp.arange(T, dtype=jnp.int32)
    projected = everything(lengths, queries, keys, values, out_weight)
    return jnp.where((token < lengths[0])[None, :, None], projected, jnp.bfloat16(0))


def solution(mesh):
    tokens = P("bucket", ("seq", "tensor"), None)
    return jax.shard_map(
        shards,
        mesh=mesh,
        in_specs=(tokens, tokens, tokens, P("bucket"), P(("seq", "bucket"), "tensor")),
        out_specs=tokens,
        check_vma=False,
    )
```
